32 devices in a mesh: rep: 2 (over x), zero: 16 (over z, y, core).
Axes of the slice: x: 2, y: 2, z: 4, core: 2. Of those that a mesh axis runs over, the one named last changes fastest.
Arguments:
- acts: bfloat16 [256, 8192], P('rep', 'zero'), may hold values from -6 to 6
- grads_out: bfloat16 [256, 8192], P('rep', 'zero'), may hold values from -12 to 12
- act_inverse: bfloat16 [8192, 8192], P('zero'), as said below
- grad_inverse: bfloat16 [8192, 8192], P('zero'), as said below
Outputs:
- precond: float32 [8192, 8192], P('zero')
The draws below stay inside these ranges and needn't reach their ends.
Inputs may be any that keep to these rules, and one draw needn't show every extreme that they name: act_inverse is symmetric. grad_inverse is symmetric.
All inputs are finite; a program needn't handle non-finite values.
Results may differ from the reference program's by a relative error of at most 0.004.
Values may be sent and summed in bfloat16 or wider, within the bound.
A program may use at most 128 MiB of HBM per device.

```python
import math
import jax
import jax.numpy as jnp
from jax import lax

D = 8192
TOKENS = 256


def make_inverse(key):
    key_raw, key_diag = jax.random.split(key, 2)
    raw = jax.random.normal(key_raw, (D, D), jnp.float32) / math.sqrt(D)
    matrix = (raw + raw.T) * 0.5
    diagonal = jax.random.uniform(key_diag, (D,), jnp.float32, 1.5, 3.0)
    matrix = matrix + jnp.diag(diagonal)
    return matrix.astype(jnp.bfloat16)


def draw_act_inverse(key, part):
    return make_inverse(jax.random.fold_in(key, 11))


def draw_grad_inverse(key, part):
    return make_inverse(jax.random.fold_in(key, 23))


def shard_levels(key, dims, shards, smallest, largest):
    loudness = 1.0
    for dim, shards_of in shards:
        draws = jax.random.uniform(jax.random.fold_in(jax.random.fold_in(key, 6), dim), (shards_of,), jnp.float32, smallest / len(shards), largest / len(shards))
        loudness = loudness * jnp.repeat(jnp.exp(draws), dims[dim] // shards_of).reshape((-1,) + (1,) * (len(dims) - 1 - dim))
    return loudness


def scatter_about(stream_key, shape, scale, bound, cuts=(), held_as=jnp.bfloat16):
    gain = shard_levels(stream_key, shape, cuts, -0.22, 0.18) if cuts else 1.0
    entries = jax.random.normal(stream_key, shape, jnp.float32) * scale * gain
    return jnp.minimum(jnp.maximum(entries, -bound), bound).astype(held_as)


def setup_inputs(seed: int = 0) -> dict:
    splits = jax.random.split(jax.random.key(seed), 5)
    acts = scatter_about(splits[0], (TOKENS, D), 1.0, 6.0, ((0, 2), (1, 16)))
    grads_out = scatter_about(splits[1], (TOKENS, D), 2.0, 12.0, ((0, 2), (1, 16)))
    act_inverse = draw_act_inverse(jax.random.fold_in(splits[4], 71), 0)
    grad_inverse = draw_grad_inverse(jax.random.fold_in(splits[4], 71), 0)
    return {"acts": acts, "grads_out": grads_out, "act_inverse": act_inverse, "grad_inverse": grad_inverse}


def reference(acts, grads_out, act_inverse, grad_inverse):
    act_pre = jnp.dot(acts, act_inverse, preferred_element_type=jnp.float32).astype(jnp.bfloat16)
    grad_pre = jnp.dot(grads_out, grad_inverse, preferred_element_type=jnp.float32).astype(jnp.bfloat16)
    summed = lax.dot_general(grad_pre, act_pre, (((0,), (0,)), ((), ())), preferred_element_type=jnp.float32)
    return summed / jnp.float32(TOKENS)
```

```python
import jax
import jax.numpy as jnp
from jax import lax
from jax.sharding import PartitionSpec as P

NT = (((1,), (1,)), ((), ()))


def on_device(acts, grads_out, act_inverse, grad_inverse):
    group = acts.shape[0]
    total_tokens = group * lax.axis_size("rep")
    both = lax.all_gather(jnp.concatenate([acts, grads_out], 0), "zero", axis=1, tiled=True)
    act_own = lax.dot_general(
        both[:group], act_inverse, NT, preferred_element_type=jnp.float32
    ).astype(jnp.bfloat16)
    act_pre = lax.all_gather(act_own, ("rep", "zero"), axis=0)
    grad_own = lax.dot_general(
        both[group:], grad_inverse, NT, preferred_element_type=jnp.float32
    ).astype(jnp.bfloat16)
    grad_pre = lax.all_gather(grad_own, "rep", axis=0, tiled=True)
    zero = lax.axis_size("zero")
    act_pre = act_pre.reshape(-1, zero, group, act_own.shape[1]).transpose(0, 2, 1, 3)
    act_pre = act_pre.reshape(total_tokens, -1)
    summed = lax.dot_general(
        grad_pre, act_pre, (((0,), (0,)), ((), ())), preferred_element_type=jnp.float32
    )
    return summed / jnp.float32(total_tokens)


def solution(mesh):
    return jax.shard_map(
        on_device,
        mesh=mesh,
        in_specs=(P("rep", "zero"), P("rep", "zero"), P("zero", None), P("zero", None)),
        out_specs=P("zero", None),
        check_vma=False,
    )
```

```python
import functools

import jax
import jax.numpy as jnp
from jax import lax
from jax.experimental import pallas as pl
from jax.experimental.pallas import tpu as pltpu
from jax.sharding import PartitionSpec as P

NT = (((1,), (1,)), ((), ()))


def gathered(acts, grads_out, act_inverse, grad_inverse):
    group = acts.shape[0]
    total_tokens = group * lax.axis_size("rep")
    both = lax.all_gather(jnp.concatenate([acts, grads_out], 0), "zero", axis=1, tiled=True)
    act_own = lax.dot_general(
        both[:group], act_inverse, NT, preferred_element_type=jnp.float32
    ).astype(jnp.bfloat16)
    act_pre = lax.all_gather(act_own, ("rep", "zero"), axis=0)
    grad_own = lax.dot_general(
        both[group:], grad_inverse, NT, preferred_element_type=jnp.float32
    ).astype(jnp.bfloat16)
    grad_pre = lax.all_gather(grad_own, "rep", axis=0, tiled=True)
    zero = lax.axis_size("zero")
    act_pre = act_pre.reshape(-1, zero, group, act_own.shape[1]).transpose(0, 2, 1, 3)
    act_pre = act_pre.reshape(total_tokens, -1)
    summed = lax.dot_general(
        grad_pre, act_pre, (((0,), (0,)), ((), ())), preferred_element_type=jnp.float32
    )
    return summed / jnp.float32(total_tokens)


MESH = pl.DeviceIdType.MESH


def gather_kernel(
    outer, acts, grads, a_hbm, g_hbm, act_out, grad_out,
    a_rows, g_rows, held, pre, grad_pre, acc_a, acc_g,
    w_sem, send1, recv1, send2, recv2, x_send, x_recv, out_sem,
):
    width = acts.shape[1]
    zero = outer * 4
    rep = lax.axis_index("rep")
    me = lax.axis_index("zero")
    z, y, c = me // 4, (me // 2) % 2, me % 2
    other_y, other_c, other_rep = 1 - y, 1 - c, 1 - rep

    def at(dz, yy, cc):
        return ((z + dz) % outer) * 4 + yy * 2 + cc

    loads = [
        pltpu.make_async_copy(a_hbm, a_rows, w_sem.at[0]),
        pltpu.make_async_copy(g_hbm, g_rows, w_sem.at[1]),
    ]
    for load in loads:
        load.start()

    hops = list(range(1, outer))
    hops.sort(key=lambda d: min(d, outer - d))
    peers = [(rep, at(d, y, c)) for d in hops]
    peers += [(rep, at(0, other_y, c)), (rep, at(0, y, other_c)), (other_rep, me)]
    barrier = pltpu.get_barrier_semaphore()
    for peer in peers:
        pl.semaphore_signal(barrier, inc=1, device_id=peer, device_id_type=MESH)
    pl.semaphore_wait(barrier, len(peers))

    own = (acts, grads)
    sent = []

    def send1_to(q, slot, block, source, peer):
        copy = pltpu.make_async_remote_copy(
            src_ref=source, dst_ref=held.at[q, block],
            send_sem=send1.at[q, slot], recv_sem=recv1.at[q, block],
            device_id=peer, device_id_type=MESH,
        )
        copy.start()
        sent.append(copy)

    def wait1(q, block):
        pltpu.make_async_copy(held.at[q, block], held.at[q, block], recv1.at[q, block]).wait()

    z_peer = {d: (rep, at(d, y, c)) for d in hops}
    y_peer = (rep, at(0, other_y, c))
    c_peer = (rep, at(0, y, other_c))
    y_slot, c_slot = outer, 2 * outer

    for q in range(2):
        for d in hops:
            send1_to(q, d, me, own[q], z_peer[d])
        send1_to(q, y_slot, me, own[q], y_peer)
        send1_to(q, c_slot, me, own[q], c_peer)

    def columns(block):
        return pl.ds(pl.multiple_of(block * width, width), width)

    def add(q, block, value):
        if q == 0:
            acc_a[...] += lax.dot_general(
                value, a_rows[:, columns(block)], NT, preferred_element_type=jnp.float32
            )
        else:
            acc_g[...] += lax.dot_general(
                g_rows[:, columns(block)], value, NT, preferred_element_type=jnp.float32
            )

    def from_z(q, ds):
        for d in ds:
            block = at(d, y, c)
            wait1(q, block)
            send1_to(q, y_slot + d, block, held.at[q, block], y_peer)
            send1_to(q, c_slot + d, block, held.at[q, block], c_peer)

    def from_y(q):
        for d in [0] + hops:
            block = at(d, other_y, c)
            wait1(q, block)
            send1_to(q, c_slot + outer + d, block, held.at[q, block], c_peer)

    def add_mine(q):
        @pl.loop(0, outer * 2)
        def _(k):
            block = (k // 2) * 4 + (k % 2) * 2 + c

            @pl.when(block != me)
            def _():
                add(q, block, held[q, block])

    def add_partner(q):
        for yy in (y, other_y):
            for d in [0] + hops:
                wait1(q, at(d, yy, other_c))

        @pl.loop(0, outer * 2)
        def _(k):
            block = (k // 2) * 4 + (k % 2) * 2 + other_c
            add(q, block, held[q, block])

    acc_a[...] = jnp.zeros_like(acc_a)
    acc_g[...] = jnp.zeros_like(acc_g)
    loads[0].wait()
    add(0, me, acts[...])
    from_z(0, hops)
    from_y(0)
    from_z(1, hops[:-1])
    add_mine(0)
    add_partner(0)

    rep1, y1 = (rep + c) % 2, (y + 1 - c) % 2
    rep2, y2 = (rep + 1 - c) % 2, (y + c) % 2
    rep3, y3 = (rep2 + c) % 2, (y2 + 1 - c) % 2

    def send2_to(slot, block, peer):
        copy = pltpu.make_async_remote_copy(
            src_ref=pre.at[block], dst_ref=pre.at[block],
            send_sem=send2.at[slot], recv_sem=recv2.at[block],
            device_id=peer, device_id_type=MESH,
        )
        copy.start()
        sent.append(copy)

    def wait2(block):
        pltpu.make_async_copy(pre.at[block], pre.at[block], recv2.at[block]).wait()

    first_peer = (rep1, at(0, y1, c))
    second_peer = (rep2, at(0, y2, c))
    s1, s2, s3 = outer, 2 * outer, 4 * outer
    mine = rep * zero + me
    pre[mine] = acc_a[...].astype(jnp.bfloat16)

    from_z(1, hops[-1:])
    for d in hops:
        send2_to(d, mine, z_peer[d])
    send2_to(s1, mine, first_peer)
    send2_to(s2, mine, second_peer)
    send2_to(s3, mine, c_peer)

    loads[1].wait()
    add(1, me, grads[...])
    from_y(1)
    for d in hops:
        block = rep * zero + at(d, y, c)
        wait2(block)
        send2_to(s1 + d, block, first_peer)
        send2_to(s2 + d, block, second_peer)
        send2_to(s3 + d, block, c_peer)
    add_mine(1)
    add_partner(1)
    grad_pre[rep] = acc_g[...].astype(jnp.bfloat16)
    for i, d in enumerate([0] + hops):
        block = rep1 * zero + at(d, y1, c)
        wait2(block)
        send2_to(s2 + outer + d, block, second_peer)
        send2_to(s3 + outer + d, block, c_peer)
        if i == 0:
            swap = pltpu.make_async_remote_copy(
                src_ref=grad_pre.at[rep], dst_ref=grad_pre.at[rep],
                send_sem=x_send, recv_sem=x_recv,
                device_id=(other_rep, me), device_id_type=MESH,
            )
            swap.start()
    for part, (rr, yy) in enumerate(((rep2, y2), (rep3, y3))):
        for d in [0] + hops:
            block = rr * zero + at(d, yy, c)
            wait2(block)
            send2_to(s3 + (2 + part) * outer + d, block, c_peer)
    swap.wait()
    grad_done = pltpu.make_async_copy(grad_pre, grad_out, out_sem.at[0])
    grad_done.start()
    for rr in (rep, other_rep):
        for yy in (y, other_y):
            for d in [0] + hops:
                wait2(rr * zero + at(d, yy, other_c))
    act_done = pltpu.make_async_copy(pre, act_out, out_sem.at[1])
    act_done.start()
    for copy in sent:
        copy.wait_send()
    grad_done.wait()
    act_done.wait()


def product_kernel(tokens, grad_ref, act_ref, out_ref):
    reps, _, group, width = act_ref.shape
    rows = jnp.concatenate([grad_ref[r] for r in range(reps)], axis=1)
    summed = jnp.dot(
        rows, act_ref[...].reshape(reps * group, width), preferred_element_type=jnp.float32
    )
    out_ref[...] = summed / jnp.float32(tokens)


def fused(acts, grads_out, act_inverse, grad_inverse):
    group, width = acts.shape
    zero = lax.axis_size("zero")
    reps = lax.axis_size("rep")
    rows, cols = act_inverse.shape
    outer = zero // 4
    bf16, dma = jnp.bfloat16, pltpu.SemaphoreType.DMA
    vmem = pl.BlockSpec(memory_space=pltpu.VMEM)
    hbm = pl.BlockSpec(memory_space=pl.ANY)
    act_pre, grad_pre = pl.pallas_call(
        functools.partial(gather_kernel, outer),
        out_shape=(
            jax.ShapeDtypeStruct((reps * zero, group, width), bf16),
            jax.ShapeDtypeStruct((reps, width, group), bf16),
        ),
        in_specs=[vmem, vmem, hbm, hbm],
        out_specs=(hbm, hbm),
        scratch_shapes=[
            pltpu.VMEM((rows, cols), bf16),
            pltpu.VMEM((rows, cols), bf16),
            pltpu.VMEM((2, zero, group, width), bf16),
            pltpu.VMEM((reps * zero, group, width), bf16),
            pltpu.VMEM((reps, width, group), bf16),
            pltpu.VMEM((group, width), jnp.float32),
            pltpu.VMEM((width, group), jnp.float32),
            dma((2,)),
            dma((2, 4 * outer)),
            dma((2, zero)),
            dma((8 * outer,)),
            dma((reps * zero,)),
            dma,
            dma,
            dma((2,)),
        ],
        compiler_params=pltpu.CompilerParams(
            collective_id=0, has_side_effects=True, vmem_limit_bytes=48 * 1024 * 1024
        ),
    )(acts, grads_out, act_inverse, grad_inverse)
    return pl.pallas_call(
        functools.partial(product_kernel, reps * group),
        grid=(zero,),
        out_shape=jax.ShapeDtypeStruct((rows, cols), jnp.float32),
        in_specs=[
            pl.BlockSpec((reps, width, group), lambda i: (0, 0, 0)),
            pl.BlockSpec((reps, 1, group, width), lambda i: (0, i, 0, 0)),
        ],
        out_specs=pl.BlockSpec((rows, width), lambda i: (0, i)),
    )(grad_pre, act_pre.reshape(reps, zero, group, width))


def on_device(acts, grads_out, act_inverse, grad_inverse):
    whole = acts.shape[1] % 128 == 0 and acts.shape[0] % 128 == 0
    if whole and lax.axis_size("rep") == 2 and lax.axis_size("zero") % 4 == 0 and lax.axis_size("zero") > 4:
        return fused(acts, grads_out, act_inverse, grad_inverse)
    return gathered(acts, grads_out, act_inverse, grad_inverse)


def solution(mesh):
    return jax.shard_map(
        on_device,
        mesh=mesh,
        in_specs=(P("rep", "zero"), P("rep", "zero"), P("zero", None), P("zero", None)),
        out_specs=P("zero", None),
        check_vma=False,
    )
```
